32 devices in a mesh: pod: 1 (over z), data: 4 (over y), expert: 8 (over x, core).
Axes of the slice: x: 4, y: 4, z: 1, core: 2. Of those that a mesh axis runs over, the one named last changes fastest.
The devices are a block of a 4x4x8 slice.
Arguments:
- tokens: bfloat16 [131072, 768], P(('pod', 'data', 'expert'))
- routes: int32 [131072, 1], P(('pod', 'data', 'expert'))
- gates: float32 [131072, 1], P(('pod', 'data', 'expert'))
- grad_y: bfloat16 [131072, 768], P(('pod', 'data', 'expert'))
- w_in1: bfloat16 [8, 768, 3072], P('expert')
- w_in3: bfloat16 [8, 768, 3072], P('expert')
- w_out: bfloat16 [8, 3072, 768], P('expert')
Outputs:
- output 1: bfloat16 [131072, 768], P(('pod', 'data', 'expert'))
- output 2: bfloat16 [131072, 768], P(('pod', 'data', 'expert'))
- output 3: float32 [8, 768, 3072], P(('pod', 'expert'))
- output 4: float32 [8, 768, 3072], P(('pod', 'expert'))
- output 5: float32 [8, 3072, 768], P(('pod', 'expert'))
All inputs are finite; a program needn't handle non-finite values.
Results may differ from the reference program's by a relative error of at most 0.001.
Values are sent between devices in bfloat16 or wider.
A program may use at most 768 MiB of HBM per device.

```python
import functools
import jax
import jax.numpy as jnp
from jax import lax

D_MODEL = 768
D_FF = 3072
N_EXPERTS = 8
TOP_K = 1
TOK_DEV = 4096
N_DATA = 4
N_EXPERT_DEV = 8
CAP_COLD = 176
CAP_HOT = 1536
N_HOT = 2

GROUPS = N_DATA * N_EXPERT_DEV
TOK_PART = GROUPS * TOK_DEV


def hot_index_table(expert_ids):
    return jnp.where(expert_ids == 0, 0, jnp.where(expert_ids == N_EXPERTS // 2, 1, -1))


def draw_routes(key):
    key_hot, key_pos, key_base_a, key_base_b, key_step = jax.random.split(key, 5)
    n_cold = N_EXPERTS - N_HOT
    pattern = jnp.concatenate([
        jnp.zeros((CAP_HOT,), jnp.int32),
        jnp.ones((CAP_HOT,), jnp.int32),
        jnp.full((TOK_DEV - N_HOT * CAP_HOT,), -1, jnp.int32)])
    hot_of_tok = jax.random.permutation(key_hot, pattern)
    hot_slot = jax.random.randint(key_pos, (TOK_DEV, 1), 0, TOP_K)
    base_rank = jnp.minimum(jax.random.randint(key_base_a, (TOK_DEV, 1), 0, n_cold),
                            jax.random.randint(key_base_b, (TOK_DEV, 1), 0, n_cold))
    step_max = max(1, (n_cold - 1) // max(TOP_K - 1, 1))
    step_size = jax.random.randint(key_step, (TOK_DEV, 1), 1, step_max + 1)
    slot_ids = jnp.arange(TOP_K)[None, :]
    cold_rank = (base_rank + slot_ids * step_size) % n_cold
    cold_expert = cold_rank + 1 + (cold_rank + 1 >= N_EXPERTS // 2).astype(jnp.int32)
    use_hot = (hot_of_tok[:, None] >= 0) & (slot_ids == hot_slot)
    return jnp.where(use_hot, hot_of_tok[:, None] * (N_EXPERTS // 2), cold_expert).astype(jnp.int32)


def setup_inputs(seed: int = 0, part: int = 0) -> dict:
    key = jax.random.key(seed)
    key_part = jax.random.fold_in(key, part)
    key_tok, key_route, key_gate, key_grad = jax.random.split(key_part, 4)
    key_one, key_three, key_two = jax.random.split(jax.random.fold_in(key, 99991), 3)
    routes = jax.vmap(draw_routes)(jax.random.split(key_route, GROUPS)).reshape(TOK_PART, TOP_K)
    tokens = jax.random.normal(key_tok, (TOK_PART, D_MODEL), jnp.float32).astype(jnp.bfloat16)
    gates = jax.random.uniform(key_gate, (TOK_PART, TOP_K), jnp.float32, 0.5, 1.5)
    grad_y = jax.random.normal(key_grad, (TOK_PART, D_MODEL), jnp.float32).astype(jnp.bfloat16)
    w_in1 = (jax.random.normal(key_one, (N_EXPERTS, D_MODEL, D_FF), jnp.float32) * D_MODEL ** -0.5).astype(jnp.bfloat16)
    w_in3 = (jax.random.normal(key_three, (N_EXPERTS, D_MODEL, D_FF), jnp.float32) * D_MODEL ** -0.5).astype(jnp.bfloat16)
    w_out = (jax.random.normal(key_two, (N_EXPERTS, D_FF, D_MODEL), jnp.float32) * D_FF ** -0.5).astype(jnp.bfloat16)
    return dict(tokens=tokens, routes=routes, gates=gates, grad_y=grad_y, w_in1=w_in1, w_in3=w_in3, w_out=w_out)


def route_rows(routes_dev):
    flat_exp = routes_dev.reshape(-1)
    n_slots = flat_exp.shape[0]
    order = jnp.argsort(flat_exp, stable=True)
    counts = jax.ops.segment_sum(jnp.ones((n_slots,), jnp.int32), flat_exp, num_segments=N_EXPERTS)
    starts = jnp.cumsum(counts) - counts
    rank_sorted = jnp.arange(n_slots, dtype=jnp.int32) - starts[flat_exp[order]]
    slot_rank = jnp.zeros((n_slots,), jnp.int32).at[order].set(rank_sorted)
    hot_index = hot_index_table(flat_exp)
    cold_row = jnp.where((hot_index < 0) & (slot_rank < CAP_COLD), flat_exp * CAP_COLD + slot_rank, N_EXPERTS * CAP_COLD)
    hot_row = jnp.where(hot_index >= 0, hot_index * CAP_HOT + slot_rank, N_HOT * CAP_HOT)
    return cold_row, hot_row


def gather_rows(slot_rows, x_local, dy_local, gate_flat, n_rows):
    n_slots = slot_rows.shape[0]
    tok_n = x_local.shape[0]
    top_k = n_slots // tok_n
    src_tok = jnp.full((n_rows,), tok_n, jnp.int32).at[slot_rows].set(
        jnp.arange(n_slots, dtype=jnp.int32) // top_k, mode='drop')
    src_gate = jnp.zeros((n_rows,), jnp.float32).at[slot_rows].set(gate_flat, mode='drop')
    x_rows = jnp.take(x_local, src_tok, axis=0, mode='fill', fill_value=0)
    dy_rows = jnp.take(dy_local, src_tok, axis=0, mode='fill', fill_value=0)
    do_rows = (dy_rows.astype(jnp.float32) * src_gate[:, None]).astype(jnp.bfloat16)
    return x_rows, do_rows


def expert_pass(x_rows, do_rows, w_a, w_b, w_c):
    pre_a = jnp.dot(x_rows, w_a, preferred_element_type=jnp.float32).astype(jnp.bfloat16)
    pre_b = jnp.dot(x_rows, w_b, preferred_element_type=jnp.float32).astype(jnp.bfloat16)
    act_a = pre_a.astype(jnp.float32)
    act_b = pre_b.astype(jnp.float32)
    sigma_a = jax.nn.sigmoid(act_a)
    hidden = (act_a * sigma_a * act_b).astype(jnp.bfloat16)
    outs = jnp.dot(hidden, w_c, preferred_element_type=jnp.float32).astype(jnp.bfloat16)
    d_hidden = jnp.dot(do_rows, w_c.T, preferred_element_type=jnp.float32)
    d_pre_b = (d_hidden * act_a * sigma_a).astype(jnp.bfloat16)
    d_pre_a = (d_hidden * act_b * sigma_a * (1.0 + act_a * (1.0 - sigma_a))).astype(jnp.bfloat16)
    d_rows = (jnp.dot(d_pre_a, w_a.T, preferred_element_type=jnp.float32)
              + jnp.dot(d_pre_b, w_b.T, preferred_element_type=jnp.float32)).astype(jnp.bfloat16)
    grad_a = jnp.dot(x_rows.T, d_pre_a, preferred_element_type=jnp.float32)
    grad_b = jnp.dot(x_rows.T, d_pre_b, preferred_element_type=jnp.float32)
    grad_c = jnp.dot(hidden.T, do_rows, preferred_element_type=jnp.float32)
    return outs, d_rows, grad_a, grad_b, grad_c


def run_expert(operands):
    return expert_pass(*operands)


def combine(cold_rows, hot_rows, cold_vals, hot_vals, weights):
    slot_vals = (jnp.take(cold_vals, cold_rows, axis=0, mode='fill', fill_value=0)
                 + jnp.take(hot_vals, hot_rows, axis=0, mode='fill', fill_value=0))
    weighted = weights.reshape(TOK_DEV, TOP_K, 1) * slot_vals.reshape(TOK_DEV, TOP_K, D_MODEL).astype(jnp.float32)
    return jnp.sum(weighted, axis=1).astype(jnp.bfloat16)


def by_expert(buffers, n_buf, cap):
    return buffers.reshape(GROUPS, n_buf, cap, D_MODEL).transpose(1, 0, 2, 3).reshape(n_buf, GROUPS * cap, D_MODEL)


def by_device(buffers, n_buf, cap):
    return buffers.reshape(n_buf, GROUPS, cap, D_MODEL).transpose(1, 0, 2, 3).reshape(GROUPS, n_buf * cap, D_MODEL)


def reference(tokens, routes, gates, grad_y, w_in1, w_in3, w_out):
    x_dev = tokens.reshape(GROUPS, TOK_DEV, D_MODEL)
    dy_dev = grad_y.reshape(GROUPS, TOK_DEV, D_MODEL)
    gate_dev = gates.reshape(GROUPS, TOK_DEV * TOP_K)
    cold_row, hot_row = jax.vmap(route_rows)(routes.reshape(GROUPS, TOK_DEV, TOP_K))
    cold_x, cold_do = jax.vmap(functools.partial(gather_rows, n_rows=N_EXPERTS * CAP_COLD))(cold_row, x_dev, dy_dev, gate_dev)
    hot_x, hot_do = jax.vmap(functools.partial(gather_rows, n_rows=N_HOT * CAP_HOT))(hot_row, x_dev, dy_dev, gate_dev)
    hot_ids = jnp.array([0, N_EXPERTS // 2])
    cold_out, cold_dx, grad_one, grad_three, grad_two = lax.map(run_expert, (
        by_expert(cold_x, N_EXPERTS, CAP_COLD), by_expert(cold_do, N_EXPERTS, CAP_COLD), w_in1, w_in3, w_out))
    hot_out, hot_dx, hot_one, hot_three, hot_two = lax.map(run_expert, (
        by_expert(hot_x, N_HOT, CAP_HOT), by_expert(hot_do, N_HOT, CAP_HOT),
        w_in1[hot_ids], w_in3[hot_ids], w_out[hot_ids]))
    y_out = jax.vmap(combine)(cold_row, hot_row, by_device(cold_out, N_EXPERTS, CAP_COLD),
                              by_device(hot_out, N_HOT, CAP_HOT), gate_dev)
    grad_x = jax.vmap(combine)(cold_row, hot_row, by_device(cold_dx, N_EXPERTS, CAP_COLD),
                               by_device(hot_dx, N_HOT, CAP_HOT), jnp.ones_like(gate_dev))
    return (y_out.reshape(TOK_PART, D_MODEL), grad_x.reshape(TOK_PART, D_MODEL),
            grad_one.at[hot_ids].add(hot_one), grad_three.at[hot_ids].add(hot_three),
            grad_two.at[hot_ids].add(hot_two))
```

```python
import functools

import jax
import jax.numpy as jnp
from jax import lax
from jax.experimental import pallas as pl
from jax.experimental.pallas import tpu as pltpu
from jax.sharding import PartitionSpec as P

N_HOT = 2
TILE = 16
BLOCK = 256
VMEM_LIMIT = 66_000_000
MESH = pl.DeviceIdType.MESH
ANY = pl.BlockSpec(memory_space=pl.ANY)
bf16, f32, i32 = jnp.bfloat16, jnp.float32, jnp.int32


def capacities(tok_dev, n_exp):
    cap_hot = 3 * tok_dev // 8
    cap_cold = max(8, ((tok_dev - N_HOT * cap_hot) // (n_exp - N_HOT) + 7) // 8 * 8)
    return cap_cold, cap_hot


def dot(a, b, ca, cb):
    return lax.dot_general(a, b, (((ca,), (cb,)), ((), ())), preferred_element_type=f32)


def route_tables(routes, core, n_exp, cap_cold, cap_hot):
    tok = routes.shape[0]
    blocks = tok // BLOCK
    n_seg = N_HOT + n_exp
    flat = routes.reshape(blocks, BLOCK)
    half = n_exp // 2
    mine, other = jnp.where(core == 0, 0, half), jnp.where(core == 0, half, 0)
    seg = jnp.where(flat == mine, 0, jnp.where(flat == other, 1, N_HOT + flat))
    count = jnp.sum((seg[:, :, None] == jnp.arange(n_seg)[None, None, :]).astype(i32), axis=1)
    before = jnp.arange(blocks)[:, None] > jnp.arange(blocks)[None, :]
    base = jnp.sum(jnp.where(before[:, :, None], count[None], 0), axis=1)
    cap = jnp.where(jnp.arange(n_seg) < N_HOT, cap_hot, cap_cold)[None, :]
    kept = jnp.clip(cap - base, 0, count)
    tiles = jnp.where(kept > 0, (base % TILE + kept + TILE - 1) // TILE, 0)
    lower = jnp.arange(n_seg)[:, None] < jnp.arange(n_seg)[None, :]
    first = jnp.sum(jnp.where(lower[None], tiles[:, :, None], 0), axis=1)
    offset = jnp.where(jnp.arange(n_seg) < N_HOT, 0, (jnp.arange(n_seg) - N_HOT) * cap_cold)[None, :]
    dest = (offset + jnp.minimum(base, cap)) // TILE
    row = (TILE * first + base % TILE).astype(f32)
    limit = (cap - base).astype(f32)
    return seg, first, tiles, dest, row, limit


def dispatch_kernel(first_ref, tiles_ref, dest_ref, seg_ref, row_ref, x_ref, dy_ref, gate_ref,
                    mine_ref, other_ref, cold_ref, stage, *, n_seg):
    j = pl.program_id(0)

    @pl.when(j == 0)
    def _():
        for ref in (mine_ref, other_ref, cold_ref):
            @pl.loop(0, ref.shape[0] // TILE)
            def _(i):
                ref[pl.ds(pl.multiple_of(i * TILE, TILE), TILE), :] = jnp.zeros((TILE, ref.shape[1]), bf16)

    seg = seg_ref[0]
    hit = lax.broadcasted_iota(i32, (n_seg, BLOCK), 0) == seg
    upto = lax.broadcasted_iota(i32, (BLOCK, BLOCK), 0) <= lax.broadcasted_iota(i32, (BLOCK, BLOCK), 1)
    rank = dot(hit.astype(f32).astype(bf16), upto.astype(f32).astype(bf16), 1, 0)
    row, limit = row_ref[0, :, 0:1], row_ref[0, :, 1:2]
    slot = jnp.sum(jnp.where(hit & (rank <= limit), rank + row, 0.0), axis=0, keepdims=True) - 1.0
    pick = (lax.broadcasted_iota(i32, (2 * BLOCK, BLOCK), 0).astype(f32) == slot).astype(f32).astype(bf16)
    d = x_ref.shape[1]
    do = (dy_ref[...].astype(f32) * gate_ref[...]).astype(bf16)
    stage[:, :d] = dot(pick, x_ref[...], 1, 0).astype(bf16)
    stage[:, d:] = dot(pick, do, 1, 0).astype(bf16)
    for s in range(n_seg):
        ref = (mine_ref, other_ref)[s] if s < N_HOT else cold_ref
        a0, t0 = first_ref[j, s], dest_ref[j, s]

        @pl.loop(0, tiles_ref[j, s])
        def _(i):
            src = pl.ds(pl.multiple_of((a0 + i) * TILE, TILE), TILE)
            dst = pl.ds(pl.multiple_of((t0 + i) * TILE, TILE), TILE)
            ref[dst, :] = ref[dst, :] + stage[src, :]


def dispatch(tokens, grad_y, gates, tables, cap_cold, cap_hot, n_exp):
    seg, first, tiles, dest, row, limit = tables
    tok, d = tokens.shape
    blocks, n_seg = first.shape
    whole = lambda n: pl.BlockSpec((n, 2 * d), lambda j, *_: (0, 0), pipeline_mode=pl.Buffered(1))
    rows = pl.BlockSpec((BLOCK, d), lambda j, *_: (j, 0))
    sizes = (cap_hot, cap_hot, n_exp * cap_cold)
    return pl.pallas_call(
        functools.partial(dispatch_kernel, n_seg=n_seg),
        grid_spec=pltpu.PrefetchScalarGridSpec(
            num_scalar_prefetch=3, grid=(blocks,),
            in_specs=[pl.BlockSpec((1, 1, BLOCK), lambda j, *_: (j, 0, 0)),
                      pl.BlockSpec((1, n_seg, 2), lambda j, *_: (j, 0, 0)),
                      rows, rows, pl.BlockSpec((BLOCK, 1), lambda j, *_: (j, 0))],
            out_specs=[whole(n) for n in sizes],
            scratch_shapes=[pltpu.VMEM((2 * BLOCK, 2 * d), bf16)]),
        out_shape=[jax.ShapeDtypeStruct((n, 2 * d), bf16) for n in sizes],
        compiler_params=pltpu.CompilerParams(dimension_semantics=("arbitrary",), vmem_limit_bytes=VMEM_LIMIT),
        cost_estimate=pl.CostEstimate(flops=tok * 2 * BLOCK * 4 * d, bytes_accessed=tok * d * 9, transcendentals=0),
        name="dispatch",
    )(first, tiles, dest, seg[:, None, :], jnp.stack([row, limit], axis=-1), tokens, grad_y, gates)


def combine_kernel(first_ref, tiles_ref, dest_ref, seg_ref, row_ref, gate_ref, mine_ref, other_ref, cold_ref,
                   y_ref, gx_ref, stage, *, n_seg):
    j = pl.program_id(0)

    @pl.when(j == 0)
    def _():
        stage[...] = jnp.zeros_like(stage)

    for s in range(n_seg):
        ref = (mine_ref, other_ref)[s] if s < N_HOT else cold_ref
        a0, t0 = first_ref[j, s], dest_ref[j, s]

        @pl.loop(0, tiles_ref[j, s])
        def _(i):
            src = pl.ds(pl.multiple_of((t0 + i) * TILE, TILE), TILE)
            dst = pl.ds(pl.multiple_of((a0 + i) * TILE, TILE), TILE)
            stage[dst, :] = ref[src, :]

    hit = lax.broadcasted_iota(i32, (BLOCK, n_seg), 1) == seg_ref[...]
    upto = lax.broadcasted_iota(i32, (BLOCK, BLOCK), 1) <= lax.broadcasted_iota(i32, (BLOCK, BLOCK), 0)
    rank = dot(upto.astype(f32).astype(bf16), hit.astype(f32).astype(bf16), 1, 0)
    row, limit = row_ref[0, 0:1, :], row_ref[0, 1:2, :]
    slot = jnp.sum(jnp.where(hit & (rank <= limit), rank + row, 0.0), axis=1, keepdims=True) - 1.0
    pick = (lax.broadcasted_iota(i32, (BLOCK, 2 * BLOCK), 1).astype(f32) == slot).astype(f32).astype(bf16)
    d = y_ref.shape[1]
    y_ref[...] = (dot(pick, stage[:, :d], 1, 0) * gate_ref[...]).astype(bf16)
    gx_ref[...] = dot(pick, stage[:, d:], 1, 0).astype(bf16)


def combine(mine, other, cold, gates, tables):
    seg, first, tiles, dest, row, limit = tables
    blocks, n_seg = first.shape
    d = mine.shape[1] // 2
    tok = blocks * BLOCK
    whole = lambda a: pl.BlockSpec(a.shape, lambda j, *_: (0, 0), pipeline_mode=pl.Buffered(1))
    rows = pl.BlockSpec((BLOCK, d), lambda j, *_: (j, 0))
    column = pl.BlockSpec((BLOCK, 1), lambda j, *_: (j, 0))
    return pl.pallas_call(
        functools.partial(combine_kernel, n_seg=n_seg),
        grid_spec=pltpu.PrefetchScalarGridSpec(
            num_scalar_prefetch=3, grid=(blocks,),
            in_specs=[column, pl.BlockSpec((1, 2, n_seg), lambda j, *_: (j, 0, 0)), column,
                      whole(mine), whole(other), whole(cold)],
            out_specs=[rows, rows],
            scratch_shapes=[pltpu.VMEM((2 * BLOCK, 2 * d), bf16)]),
        out_shape=[jax.ShapeDtypeStruct((tok, d), bf16)] * 2,
        compiler_params=pltpu.CompilerParams(dimension_semantics=("arbitrary",), vmem_limit_bytes=VMEM_LIMIT),
        cost_estimate=pl.CostEstimate(flops=tok * 2 * BLOCK * 4 * d, bytes_accessed=tok * d * 9, transcendentals=0),
        name="combine",
    )(first, tiles, dest, seg.reshape(tok, 1), jnp.stack([row, limit], axis=1), gates, mine, other, cold)


def expert_kernel(*refs, n_src, roles, sizes, tb, sb, fc):
    refs = list(refs)
    srcs = [refs.pop(0) for _ in range(n_src)]
    n_w = len(roles)
    sources = [[refs.pop(0) for _ in range(3)] for _ in range(n_w)]
    outs = [refs.pop(0) for _ in range(n_src)]
    g1_ref, g3_ref, g2_ref = refs[:3]
    xs, xt, dt, acc, g2t, w1b, w3b, w2b, sem_x, sem_w = refs[3:]
    f, t = pl.program_id(0), pl.program_id(1)
    nf, nt = pl.num_programs(0), pl.num_programs(1)
    d = g1_ref.shape[0]

    def weight_copies(source, chunk, slot):
        w1, w3, w2 = source
        at = pl.ds(pl.multiple_of(chunk * fc, fc), fc)
        return [pltpu.make_async_copy(w1.at[:, at], w1b.at[slot], sem_w.at[slot, 0]),
                pltpu.make_async_copy(w3.at[:, at], w3b.at[slot], sem_w.at[slot, 1]),
                pltpu.make_async_copy(w2.at[at, :], w2b.at[slot], sem_w.at[slot, 2])]

    def fetch(chunk, slot):
        for pred, source in zip(roles, sources):
            def go(source=source):
                for c in weight_copies(source, chunk, slot):
                    c.start()
            if pred is None:
                go()
            else:
                pl.when(pred())(go)

    @pl.when(jnp.logical_and(f == 0, t == 0))
    def _():
        fetch(0, 0)
        copies, at = [], 0
        for i, src in enumerate(srcs):
            copies.append(pltpu.make_async_copy(src, xs.at[pl.ds(at, sizes[i]), :], sem_x.at[i]))
            at += sizes[i]
        for c in copies:
            c.start()
        for c in copies:
            c.wait()

    slot = lax.rem(f, 2)

    @pl.when(t == 0)
    def _():
        for c in weight_copies(sources[0], f, slot):
            c.wait()

        @pl.when(f + 1 < nf)
        def _():
            fetch(f + 1, 1 - slot)

        g1_ref[...] = jnp.zeros_like(g1_ref)
        g3_ref[...] = jnp.zeros_like(g3_ref)
        g2t[...] = jnp.zeros_like(g2t)

    rows = pl.ds(pl.multiple_of(t * tb, tb), tb)

    @pl.when(f == 0)
    def _():
        xt[t] = xs[rows, :d].T
        dt[t] = xs[rows, d:].T
        acc[rows, :] = jnp.zeros((tb, 2 * d), f32)

    w1, w3, w2 = w1b[slot], w3b[slot], w2b[slot]
    hs, das, dbs = [], [], []
    for i in range(tb // sb):
        part = pl.ds(pl.multiple_of(t * tb + i * sb, sb), sb)
        x, do = xs[part, :d], xs[part, d:]
        a = dot(x, w1, 1, 0).astype(bf16).astype(f32)
        b = dot(x, w3, 1, 0).astype(bf16).astype(f32)
        dh = dot(do, w2, 1, 1)
        sg = jax.nn.sigmoid(a)
        h = (a * sg * b).astype(bf16)
        db = (dh * a * sg).astype(bf16)
        da = (dh * b * sg * (1.0 + a * (1.0 - sg))).astype(bf16)
        hs.append(h), das.append(da), dbs.append(db)
        acc[part, :d] += dot(h, w2, 1, 0)
        acc[part, d:] += dot(da, w1, 1, 1) + dot(db, w3, 1, 1)
    h, da, db = jnp.concatenate(hs), jnp.concatenate(das), jnp.concatenate(dbs)
    xT, dT = xt[t], dt[t]
    g1_ref[...] += dot(xT, da, 1, 0)
    g3_ref[...] += dot(xT, db, 1, 0)
    g2t[...] += dot(dT, h, 1, 0)

    @pl.when(t == nt - 1)
    def _():
        g2_ref[...] = g2t[...].T

    at = 0
    for i, out in enumerate(outs):
        n = sizes[i] // tb

        @pl.when(jnp.logical_and(f == nf - 1, jnp.logical_and(t >= at, t < at + n)))
        def _():
            out[...] = acc[rows, :].astype(bf16)
        at += n


def expert_pass(srcs, weights, roles, tb, sb, fc, name):
    d, ff = weights[0][0].shape
    sizes = [s.shape[0] for s in srcs]
    total = sum(sizes)
    nf, nt = ff // fc, total // tb
    specs, at = [], 0
    for n in sizes:
        n_b = n // tb

        def index(f, t, at=at, n_b=n_b):
            return jnp.where(f == nf - 1, jnp.clip(t - at, 0, n_b - 1), 0), 0
        specs.append(pl.BlockSpec((tb, 2 * d), index))
        at += n_b
    column = pl.BlockSpec((d, fc), lambda f, t: (0, f))
    res = pl.pallas_call(
        functools.partial(expert_kernel, n_src=len(srcs), roles=roles, sizes=sizes, tb=tb, sb=sb, fc=fc),
        grid=(nf, nt),
        in_specs=[ANY] * (len(srcs) + 3 * len(weights)),
        out_specs=specs + [column, column, pl.BlockSpec((fc, d), lambda f, t: (f, 0))],
        out_shape=[jax.ShapeDtypeStruct(s.shape, bf16) for s in srcs] + [
            jax.ShapeDtypeStruct((d, ff), f32)] * 2 + [jax.ShapeDtypeStruct((ff, d), f32)],
        scratch_shapes=[pltpu.VMEM((total, 2 * d), bf16), pltpu.VMEM((nt, d, tb), bf16), pltpu.VMEM((nt, d, tb), bf16),
                        pltpu.VMEM((total, 2 * d), f32), pltpu.VMEM((d, fc), f32),
                        pltpu.VMEM((2, d, fc), bf16), pltpu.VMEM((2, d, fc), bf16), pltpu.VMEM((2, fc, d), bf16),
                        pltpu.SemaphoreType.DMA((len(srcs),)), pltpu.SemaphoreType.DMA((2, 3))],
        compiler_params=pltpu.CompilerParams(
            dimension_semantics=("arbitrary", "arbitrary"), vmem_limit_bytes=VMEM_LIMIT),
        cost_estimate=pl.CostEstimate(flops=total * d * ff * 18, bytes_accessed=d * ff * 18 + total * d * 8,
                                      transcendentals=total * ff),
        name=name,
    )(*srcs, *[w for group in weights for w in group])
    return res[:len(srcs)], res[len(srcs):]


def gradient_kernel(*refs, nx, ny, lag):
    g, c, o = refs[0:3], refs[3:6], refs[6:9]
    (xsa, xsb, xfa, xfb, la, lb, yha, yhb, yfa, yfb, aga, agb,
     s_xs, s_xr, s_loc, s_agl, s_own, s_ags, s_agr, s_rs, s_rr, s_hs, s_hr, s_fs, s_fr, s_gs, s_gr) = refs[9:]
    q, r = lax.axis_index("data"), lax.axis_index("expert")
    x, core = r // 2, lax.rem(r, 2)
    n_dev = 2 * nx
    owner = jnp.where(core == 0, 0, n_dev // 2)
    is_hot = jnp.logical_or(r == 0, r == n_dev // 2)
    unit = [ref.shape[0] // (nx * ny) for ref in g]
    kinds = range(3)

    def pick(a, b, kind, *lead):
        return a.at[(*lead, kind)] if kind < 2 else b.at[lead]

    def rows(kind, j, i, lo=0, n=None):
        u = unit[kind]
        start = pl.multiple_of((lax.rem(j + 4 * ny, ny) * nx + lax.rem(i + 4 * nx, nx)) * u + lo, 8)
        return pl.ds(start, u if n is None else n)

    def half(kind, which):
        h = unit[kind] // 2
        return pl.ds(which * h, h)

    def remote(src, dst, send, recv, **where):
        return pltpu.make_async_remote_copy(src_ref=src, dst_ref=dst, send_sem=send, recv_sem=recv,
                                            device_id=where, device_id_type=MESH)

    def add(dst, a, b, n, step):
        @pl.loop(0, n // step)
        def _(i):
            at = pl.ds(pl.multiple_of(i * step, 8), step)
            dst[at, :] = a[at, :] + b[at, :]

    step_rows = [8, 8, 32]
    east = lambda d: lax.rem(r + (2 if d == 0 else n_dev - 2), n_dev)
    north = lambda d: lax.rem(q + (1 if d == 0 else ny - 1), ny)
    rel_of = ((2, 1), (3, 0))

    def chunk(d, s):
        return x - 1 - s if d == 0 else x + 1 + s

    def local(d, s, jj, kind):
        return pltpu.make_async_copy(g[kind].at[rows(kind, q + rel_of[d][jj], chunk(d, s)), :],
                                     pick(la, lb, kind, d), s_loc.at[d, kind])

    def x_send(d, s, jj, kind):
        k = jj * 3 + kind
        src = (g[kind].at[rows(kind, q + rel_of[d][jj], chunk(d, 0)), :] if s == 0
               else pick(xsa, xsb, kind, d, s - 1, jj))
        return remote(src, pick(xsa, xsb, kind, d, s, jj), s_xs.at[d, s, k], s_xr.at[d, s, k], expert=east(d))

    def ag_load(kind, i):
        u = unit[kind]
        return pltpu.make_async_copy(c[kind].at[pl.ds(i * u, u), :], pick(aga, agb, kind, i), s_agl.at[kind, i])

    def ag_own(kind, i):
        return pltpu.make_async_copy(pick(aga, agb, kind, i), o[kind].at[rows(kind, q, i), :], s_own.at[kind, i])

    def ag_send(d, kind, i):
        return remote(pick(aga, agb, kind, i), o[kind].at[rows(kind, q, i), :],
                      s_ags.at[d, kind, i], s_agr.at[d, kind, i], data=north(d))

    def ag_relay(d, kind, i):
        h = unit[kind] // 2
        from_q = q - 1 if d == 0 else q + 1
        at = rows(kind, from_q, i, d * h, h)
        return remote(o[kind].at[at, :], o[kind].at[at, :], s_rs.at[d, kind, i], s_rr.at[d, kind, i], data=north(d))

    def gather_send(kind):
        return remote(pick(xfa, xfb, kind, 0), aga.at[x, kind] if kind < 2 else agb.at[x],
                      s_gs.at[kind], s_gr.at[kind, x], expert=owner)

    def y_half(d, kind):
        return remote(pick(xfa, xfb, kind, 2).at[half(kind, d), :], pick(yha, yhb, kind, d),
                      s_hs.at[d, kind], s_hr.at[d, kind], data=north(d))

    def y_full(d, kind):
        return remote(pick(xfa, xfb, kind, 1 if d == 0 else 3), pick(yfa, yfb, kind, d),
                      s_fs.at[d, kind], s_fr.at[d, kind], data=north(d))

    def ag_start(kind, i):
        ag_own(kind, i).start()
        for d in range(2):
            ag_send(d, kind, i).start()

    def ag_pass_on(kind, i):
        for d in range(2):
            ag_send(d, kind, i).wait_recv()
            ag_relay(d, kind, i).start()

    items = [(kind, i) for i in range(nx) for kind in kinds]

    order = {(d, kind): [] for d in range(2) for kind in kinds}
    rounds = []
    for n in range(6 + 3 * lag):
        now = []
        for s in (3, 2, 1, 0):
            k = n - lag * s
            if 0 <= k < 6:
                now.append((s, k // 3, k % 3))
        rounds.append(now)
        for s, jj, kind in now:
            if s > 0:
                for d in range(2):
                    order[d, kind].append((s, jj))

    position = {key: 0 for key in order}
    for d in range(2):
        for kind in kinds:
            s, jj = order[d, kind][0]
            local(d, s, jj, kind).start()

    @pl.when(jnp.logical_not(is_hot))
    def _():
        for kind, i in items:
            ag_load(kind, i).start()

    passed = 0
    for n, now in enumerate(rounds):
        for s, jj, kind in now:
            for d in range(2):
                if s == 0:
                    x_send(d, 0, jj, kind).start()
                    continue
                x_send(d, s - 1, jj, kind).wait_recv()
                local(d, s, jj, kind).wait()
                slot = pick(xsa, xsb, kind, d, s - 1, jj)
                dst = slot if s < 3 else pick(xfa, xfb, kind, rel_of[d][jj])
                add(dst, slot, pick(la, lb, kind, d), unit[kind], step_rows[kind])
                if s < 3:
                    x_send(d, s, jj, kind).start()
                position[d, kind] += 1
                if position[d, kind] < len(order[d, kind]):
                    s2, jj2 = order[d, kind][position[d, kind]]
                    local(d, s2, jj2, kind).start()
            if s == 3 and jj == 0:
                for d in range(2):
                    y_half(d, kind).start()
            if s == 3 and jj == 1:
                for d in range(2):
                    y_half(d, kind).wait_recv()
                    piece = pick(xfa, xfb, kind, 1 if d == 0 else 3).at[half(kind, d), :]
                    add(piece, piece, pick(yha, yhb, kind, d), unit[kind] // 2, 8)
                    y_full(d, kind).start()

        @pl.when(jnp.logical_not(is_hot))
        def _():
            if n == 0:
                for kind, i in items:
                    ag_load(kind, i).wait()
                    ag_start(kind, i)
            elif n <= len(items):
                ag_pass_on(*items[n - 1])
        passed = min(n, len(items))

    @pl.when(jnp.logical_not(is_hot))
    def _():
        for kind, i in items[passed:]:
            ag_pass_on(kind, i)

    for kind in kinds:
        for d in range(2):
            y_full(d, kind).wait_recv()
        piece = pick(xfa, xfb, kind, 0)
        add(piece, piece, pick(yfa, yfb, kind, 0), unit[kind], step_rows[kind])
        mine = r == owner

        @pl.when(mine)
        def _():
            add(pick(aga, agb, kind, 0), piece, pick(yfa, yfb, kind, 1), unit[kind], step_rows[kind])

        @pl.when(jnp.logical_not(mine))
        def _():
            add(piece, piece, pick(yfa, yfb, kind, 1), unit[kind], step_rows[kind])
            gather_send(kind).start()

    @pl.when(is_hot)
    def _():
        for kind in kinds:
            for i in range(nx):
                if i == 0:
                    @pl.when(r != 0)
                    def _():
                        pltpu.make_async_remote_copy(
                            src_ref=pick(xfa, xfb, kind, 0), dst_ref=pick(aga, agb, kind, i), send_sem=s_gs.at[kind],
                            recv_sem=s_gr.at[kind, i], device_id={"expert": owner}, device_id_type=MESH).wait_recv()
                else:
                    pltpu.make_async_remote_copy(
                        src_ref=pick(xfa, xfb, kind, 0), dst_ref=pick(aga, agb, kind, i), send_sem=s_gs.at[kind],
                        recv_sem=s_gr.at[kind, i], device_id={"expert": owner}, device_id_type=MESH).wait_recv()
                ag_start(kind, i)
        for kind in kinds:
            for i in range(nx):
                ag_pass_on(kind, i)

    for d in range(2):
        for kind in kinds:
            for jj in range(2):
                for s in range(3):
                    x_send(d, s, jj, kind).wait_send()
            y_half(d, kind).wait_send()
            y_full(d, kind).wait_send()
            for i in range(nx):
                ag_send(d, kind, i).wait_send()
                ag_relay(d, kind, i).wait()
    for kind in kinds:
        for i in range(nx):
            ag_own(kind, i).wait()

        @pl.when(r != owner)
        def _():
            gather_send(kind).wait_send()


def finish_gradients(hot, cold, nx, ny, lag=2):
    ua, ub = hot[0].shape[0] // (nx * ny), hot[2].shape[0] // (nx * ny)
    wa, wb = hot[0].shape[1], hot[2].shape[1]
    va = lambda *lead: pltpu.VMEM((*lead, 2, ua, wa), f32)
    vb = lambda *lead: pltpu.VMEM((*lead, ub, wb), f32)
    sem = lambda *n: pltpu.SemaphoreType.DMA(n)
    sent = sum(h.size * 4 for h in hot)
    return pl.pallas_call(
        functools.partial(gradient_kernel, nx=nx, ny=ny, lag=lag),
        in_specs=[ANY] * 6, out_specs=[ANY] * 3,
        out_shape=[jax.ShapeDtypeStruct(h.shape, f32) for h in hot],
        scratch_shapes=[
            va(2, 3, 2), vb(2, 3, 2), va(4), vb(4), va(2), vb(2),
            pltpu.VMEM((2, 2, ua // 2, wa), f32), pltpu.VMEM((2, ub // 2, wb), f32), va(2), vb(2),
            va(nx), vb(nx),
            sem(2, 3, 6), sem(2, 3, 6), sem(2, 3), sem(3, nx), sem(3, nx), sem(2, 3, nx), sem(2, 3, nx), sem(2, 3, nx),
            sem(2, 3, nx), sem(2, 3), sem(2, 3), sem(2, 3), sem(2, 3), sem(3), sem(3, nx)],
        compiler_params=pltpu.CompilerParams(has_side_effects=True, vmem_limit_bytes=VMEM_LIMIT),
        cost_estimate=pl.CostEstimate(flops=sent, bytes_accessed=4 * sent, transcendentals=0),
        name="finish_gradients",
    )(*hot, *cold)


def solution(mesh):
    n_dev, ny = mesh.shape["expert"], mesh.shape["data"]
    nx = n_dev // 2
    assert nx == 4 and ny == 4
    row_spec = P(("pod", "data", "expert"), None)
    w_spec = P("expert", None, None)
    grad_spec = P(("pod", "expert"), None, None)
    h0, h1 = 0, n_dev // 2

    def body(tokens, routes, gates, grad_y, w_in1, w_in3, w_out):
        tok, d = tokens.shape
        ff = w_in1.shape[2]
        n_exp = w_in1.shape[0] * n_dev
        r = lax.axis_index("expert")
        cap_cold, cap_hot = capacities(tok, n_exp)
        own = (w_in1[0], w_in3[0], w_out[0])

        send = lambda ws, pairs: [lax.ppermute(w, "expert", pairs) for w in ws]
        p1 = send(own, [(h0, h0 + 2), (h1, h1 + 3)])
        p2 = send(own, [(h0, n_dev - 2), (h1, h1 - 1)])
        p0 = send(own, [(h1, h1 + 1)])
        p3 = send((p1[0], p1[2]), [(h0 + 2, h1), (h1 + 3, h0 + 1)])
        p4 = send((p2[1],), [(n_dev - 2, h1), (h1 - 1, h0 + 1)])
        hot_w = [own, p0, p1, p2, (p3[0], p4[0], p3[1])]

        def role(*members):
            def test():
                me = lax.axis_index("expert")
                hit = me == members[0]
                for m in members[1:]:
                    hit = jnp.logical_or(hit, me == m)
                return hit
            return test
        roles = [role(h0), role(h1 + 1), role(h0 + 2, h1 + 3), role(n_dev - 2, h1 - 1), role(h1, h0 + 1)]

        tables = route_tables(routes, lax.rem(r, 2), n_exp, cap_cold, cap_hot)
        mine, other, cold = dispatch(tokens, grad_y, gates, tables, cap_cold, cap_hot, n_exp)
        swap = [(i, i ^ 1) for i in range(n_dev)]
        guest = lax.ppermute(other, "expert", swap)
        a2a = lambda v: lax.all_to_all(v.reshape(n_dev, cap_cold, 2 * d), "expert", 0, 0, tiled=True).reshape(v.shape)
        recv = a2a(cold)

        (cold_out,), cold_g = expert_pass([recv], [own], [None], recv.shape[0], recv.shape[0] // 2, 512, "cold")
        part = [lax.psum_scatter(v, "data", scatter_dimension=0, tiled=True) for v in cold_g]
        back = a2a(cold_out)
        (mine_out, guest_out), hot_g = expert_pass([mine, guest], hot_w, roles, 512, 512, 512, "hot")
        other_out = lax.ppermute(guest_out, "expert", swap)
        grads = finish_gradients(hot_g, part, nx, ny)
        y, gx = combine(mine_out, other_out, back, gates, tables)
        return (y, gx, *[v[None] for v in grads])

    return jax.shard_map(body, mesh=mesh,
                         in_specs=(row_spec, row_spec, row_spec, row_spec, w_spec, w_spec, w_spec),
                         out_specs=(row_spec, row_spec, grad_spec, grad_spec, grad_spec),
                         check_vma=False)
```
